32 devices in a mesh: batch: 2 (over x), row: 4 (over z), col: 4 (over y, core).
Axes of the slice: x: 2, y: 2, z: 4, core: 2. Of those that a mesh axis runs over, the one named last changes fastest.
Arguments:
- spd_blocks: float32 [96, 128, 6144], P(('batch', 'row'), None, 'col'), parts along dimension 0
Outputs:
- output: float32 [96, 128, 6144], P(('batch', 'row'), None, 'col'), parts along dimension 0
There are 2 independent parts. The reference program is written for one: setup_inputs(seed, part) draws one part's arguments, and reference() takes and returns one part's arrays. A program takes and returns all parts, laid end to end along the dimension named above; each array names one.
All inputs are finite; a program needn't handle non-finite values.
Results may differ from the reference program's by a relative error of at most 0.001.
Values are sent between devices in bfloat16 or wider.
A program may use at most 1 GiB of HBM per device.

```python
import math
import jax
import jax.numpy as jnp
from jax import lax

BLOCK = 128
ORDER = 6144
ROW_DEVS = 4
COL_DEVS = 4

BLOCK_COUNT = ORDER // BLOCK


def to_logical(a_cyc):
    by_rows = a_cyc.reshape(ROW_DEVS, BLOCK_COUNT // ROW_DEVS, BLOCK, ORDER).transpose(1, 0, 2, 3)
    by_cols = by_rows.reshape(ORDER, COL_DEVS, BLOCK_COUNT // COL_DEVS, BLOCK).transpose(0, 2, 1, 3)
    return by_cols.reshape(ORDER, ORDER)


def to_cyclic(matrix):
    by_rows = matrix.reshape(BLOCK_COUNT // ROW_DEVS, ROW_DEVS, BLOCK, ORDER).transpose(1, 0, 2, 3)
    by_cols = by_rows.reshape(ORDER, BLOCK_COUNT // COL_DEVS, COL_DEVS, BLOCK).transpose(0, 2, 1, 3)
    return by_cols.reshape(BLOCK_COUNT, BLOCK, ORDER)


def setup_inputs(seed: int = 0, part: int = 0) -> dict:
    rng_key = jax.random.fold_in(jax.random.key(seed), part)
    gauss_draw = jax.random.normal(rng_key, (ORDER, ORDER), jnp.float32)
    sym_part = (gauss_draw + gauss_draw.T) * math.sqrt(0.5 / ORDER)
    matrix = (sym_part + 2.2 * jnp.eye(ORDER, dtype=jnp.float32)) * ORDER
    return {"spd_blocks": to_cyclic(matrix)}


def reference(spd_blocks):
    trailing = to_logical(spd_blocks)
    columns = []
    for step_idx in range(BLOCK_COUNT):
        diag_fac = jnp.tril(jnp.linalg.cholesky(trailing[:BLOCK, :BLOCK]))
        pieces = [jnp.zeros((step_idx * BLOCK, BLOCK), jnp.float32), diag_fac]
        if step_idx + 1 < BLOCK_COUNT:
            panel_f32 = lax.linalg.triangular_solve(diag_fac, trailing[BLOCK:, :BLOCK], left_side=False, lower=True, transpose_a=True)
            pieces.append(panel_f32)
            panel_b16 = panel_f32.astype(jnp.bfloat16)
            trailing = trailing[BLOCK:, BLOCK:] - jnp.dot(panel_b16, panel_b16.T, preferred_element_type=jnp.float32)
        columns.append(jnp.concatenate(pieces, axis=0))
    return to_cyclic(jnp.concatenate(columns, axis=1))
```

```python
import functools
import jax
import jax.numpy as jnp
from jax import lax
from jax.experimental import pallas as pl
from jax.experimental.pallas import tpu as pltpu
from jax.sharding import PartitionSpec as P

B = 128
NBLK = 48
G = 4
NLOC = 12
CH = 3
NCH = NLOC // CH
CR = CH * B
PANEL = 32
MESH = pl.DeviceIdType.MESH
NT = (((1,), (1,)), ((), ()))
TN = (((0,), (0,)), ((), ()))
F32 = jnp.float32
BF16 = jnp.bfloat16


def split3(x):
    hi = x.astype(BF16)
    rest = x - hi.astype(F32)
    mid = rest.astype(BF16)
    low = (rest - mid.astype(F32)).astype(BF16)
    return hi, mid, low


def left6(x, axis):
    hi, mid, low = split3(x)
    return jnp.concatenate([hi, mid, low, hi, mid, hi], axis=axis)


def right6(x, axis):
    hi, mid, low = split3(x)
    return jnp.concatenate([low, mid, hi, mid, hi, hi], axis=axis)


def dot(a, b, dims):
    return lax.dot_general(a, b, dims, preferred_element_type=F32)


def factor_panel(w, lane0):
    n = w.shape[0]
    cols = jnp.stack([jnp.broadcast_to(w[:, lane0 + j:lane0 + j + 1], (n, B)) for j in range(n)])
    sub = lax.broadcasted_iota(jnp.int32, (8, 2 * B), 0)
    groups = [w[8 * g:8 * g + 8] for g in range(n // 8)]
    for j in range(n):
        g0, s = j // 8, j % 8
        if s == 0 and j:
            cols = cols[:, 8:]
        inv = lax.rsqrt(cols[0, s:s + 1])
        fac = cols[0] * inv
        if j + 1 < n:
            cols = cols[1:] - fac[None] * fac[s + 1:, None, :]
        pivot = groups[g0][s:s + 1] * jnp.concatenate([inv, inv], axis=1)
        fac2 = jnp.concatenate([fac, fac], axis=1)
        head = groups[g0]
        groups[g0] = jnp.where(sub == s, pivot, jnp.where(sub > s, head - fac2[:8] * pivot, head))
        for g in range(g0 + 1, n // 8):
            groups[g] = groups[g] - fac2[8 * (g - g0):8 * (g - g0) + 8] * pivot
    return jnp.concatenate(groups, axis=0)


def factor_block(a):
    r = lax.broadcasted_iota(jnp.int32, (B, B), 0)
    c = lax.broadcasted_iota(jnp.int32, (B, B), 1)
    w = jnp.concatenate([a, jnp.where(r == c, 1.0, 0.0).astype(F32)], axis=1)
    done = []
    for p in range(B // PANEL):
        f = factor_panel(w[:PANEL], PANEL * p)
        done.append(f)
        if p + 1 < B // PANEL:
            w = w[PANEL:] - dot(left6(f[:, :B], 0), right6(f, 0), TN)[PANEL * (p + 1):]
    f = jnp.concatenate(done, axis=0)
    return f[:, :B], f[:, B:]


def kernel(a_ref, s_ref, rp, cp, cb, linv, ld, a_s, mcat, rhs_s, in_sem,
           inv_r, inv_s, cb_r, cb_s, rp_r, rp_s, cp_r, cp_s):
    bt = lax.axis_index("batch")
    r = lax.axis_index("row")
    c = lax.axis_index("col")

    def rows(i, n=B):
        return pl.ds(pl.multiple_of(i * B, B), n)

    def phase(k):
        return lax.div(k, 12)

    def base(k):
        p = phase(k)
        return 144 * p - 18 * p * (p - 1) + (k - 12 * p) * (12 - 3 * p)

    def chunk(k, q):
        return rows(base(k) + CH * (q - phase(k)), CR)

    def rcopy(buf, where, ssem, rsem, dev):
        return pltpu.make_async_remote_copy(
            src_ref=buf.at[where, :], dst_ref=buf.at[where, :], send_sem=ssem, recv_sem=rsem,
            device_id=dev, device_id_type=MESH)

    def inv_copy(k, j, dev):
        return rcopy(linv, rows(k), inv_s.at[k * 3 + j], inv_r.at[k], dev)

    def cb_copy(k, j, dev):
        return rcopy(cb, rows(k), cb_s.at[k * 4 + j], cb_r.at[k], dev)

    def rp_copy(k, q, j, dev):
        return rcopy(rp, chunk(k, q), rp_s.at[(k * 3 + j) * NCH + q], rp_r.at[k * NCH + q], dev)

    def cp_copy(k, q, j, dev):
        return rcopy(cp, chunk(k, q), cp_s.at[(k * 2 + j) * NCH + q], cp_r.at[k * NCH + q], dev)

    dest_a = jnp.where(lax.rem(c, 2) == 0, c + 1, c - 1)
    dest_b = jnp.where(c < 2, 2, 1)
    dest_e = jnp.where(c < 2, 3, 0)
    is_diag = r == c
    relays = (r == dest_b) & (r != c)

    def inv_send(k):
        return k < NBLK - 1

    load = pltpu.make_async_copy(a_ref, s_ref, in_sem)
    load.start()
    load.wait()

    def step(it, carry):
        k = it - 1
        kk = jnp.maximum(k, 0)
        kr = lax.rem(kk, G)
        nr = lax.rem(it, G)
        p = phase(kk)
        tk = lax.div(kk, G)
        tn = lax.div(it, G)

        @pl.when((k >= 0) & (c == kr))
        def _():
            @pl.when(r != kr)
            def _():
                inv_copy(kk, 0, (bt, kr, c)).wait_recv()

            mcat[...] = right6(linv[rows(kk), :], 1)

            @pl.when(r == nr)
            def _():
                x = dot(left6(s_ref[rows(tn), rows(tk)], 1), mcat[...], NT)
                cb[rows(kk), :] = x.astype(BF16)
                cb_copy(kk, 0, (bt, nr, nr)).start()

                @pl.when(k <= NBLK - 3)
                def _():
                    for j in range(1, G):
                        cb_copy(kk, j, (bt, lax.rem(nr + j, G), nr)).start()

            def solve(q, carry):
                x = s_ref[rows(CH * q, CR), rows(tk)]
                y = dot(left6(x, 1), mcat[...], NT)
                t = lax.broadcasted_iota(jnp.int32, (CR, B), 0) // B + CH * q
                below = t * G + r > kk
                s_ref[rows(CH * q, CR), rows(tk)] = jnp.where(below, y, x)
                rp[chunk(kk, q), :] = jnp.where(below, y, 0.0).astype(BF16)

                @pl.when(k <= NBLK - 3)
                def _():
                    for j in range(3):
                        rp_copy(kk, q, j, (bt, r, lax.rem(kr + 1 + j, G))).start()

                return carry

            lax.fori_loop(p, NCH, solve, 0)

        @pl.when((r == nr) & (c == nr))
        def _():
            a_s[...] = s_ref[rows(tn), rows(tn)]

            @pl.when(k >= 1)
            def _():
                kp = jnp.maximum(k - 1, 0)
                blk = rp[rows(base(kp) + tn - CH * phase(kp)), :]
                a_s[...] -= dot(blk, blk, NT)

            @pl.when(k >= 0)
            def _():
                cb_copy(kk, 0, (bt, r, kr)).wait_recv()
                blk = cb[rows(kk), :]
                a_s[...] -= dot(blk, blk, NT)

            u, m = factor_block(a_s[...])
            linv[rows(it), :] = m

            @pl.when(it < NBLK - 1)
            def _():
                for j in range(3):
                    inv_copy(it, j, (bt, lax.rem(nr + 1 + j, G), c)).start()

            low = jnp.transpose(u)
            i0 = lax.broadcasted_iota(jnp.int32, (B, B), 0)
            i1 = lax.broadcasted_iota(jnp.int32, (B, B), 1)
            ld[rows(tn), :] = jnp.where(i0 >= i1, low, 0.0)

        @pl.when((k >= 0) & (k <= NBLK - 3))
        def _():
            @pl.when((c == nr) & (r != nr))
            def _():
                cb_copy(kk, 0, (bt, nr, kr)).wait_recv()

            def take(q, carry):
                @pl.when(c != kr)
                def _():
                    rp_copy(kk, q, 0, (bt, r, kr)).wait_recv()

                @pl.when(is_diag & (k <= NBLK - 4))
                def _():
                    for j, d in ((0, dest_b), (1, dest_a)):
                        pltpu.make_async_remote_copy(
                            src_ref=rp.at[chunk(kk, q), :], dst_ref=cp.at[chunk(kk, q), :],
                            send_sem=cp_s.at[(kk * 2 + j) * NCH + q], recv_sem=cp_r.at[kk * NCH + q],
                            device_id=(bt, d, c), device_id_type=MESH).start()

                @pl.when(c == nr)
                def _():
                    s_ref[rows(CH * q, CR), rows(tn)] -= dot(rp[chunk(kk, q), :], cb[rows(kk), :], NT)

                return carry

            lax.fori_loop(p, NCH, take, 0)

        @pl.when((k >= 1) & (k <= NBLK - 3))
        def _():
            kp = jnp.maximum(k - 1, 0)
            pp = phase(kp)

            def arrive(q, carry):
                @pl.when(jnp.logical_not(is_diag))
                def _():
                    cp_copy(kp, q, 0, (bt, c, c)).wait_recv()

                @pl.when(relays)
                def _():
                    cp_copy(kp, q, 0, (bt, dest_e, c)).start()

                return carry

            lax.fori_loop(pp, NCH, arrive, 0)

            def by_col(cq, carry):
                @pl.when(is_diag)
                def _():
                    rhs_s[...] = rp[chunk(kp, cq), :]

                @pl.when(jnp.logical_not(is_diag))
                def _():
                    rhs_s[...] = cp[chunk(kp, cq), :]

                @pl.when((c == kr) & (lax.div(tk, CH) == cq))
                def _():
                    rhs_s[rows(lax.rem(tk, CH)), :] = jnp.zeros((B, B), BF16)

                def by_row(rq, carry):
                    s_ref[rows(CH * rq, CR), rows(CH * cq, CR)] -= dot(rp[chunk(kp, rq), :], rhs_s[...], NT)
                    return carry

                return lax.fori_loop(cq, NCH, by_row, carry)

            lax.fori_loop(pp, NCH, by_col, 0)

        return carry

    lax.fori_loop(0, NBLK, step, 0)

    def drain(k, carry):
        kr = lax.rem(k, G)
        nr = lax.rem(k + 1, G)
        p = phase(k)

        @pl.when((r == kr) & (c == kr) & (k < NBLK - 1))
        def _():
            for j in range(3):
                inv_copy(k, j, (bt, lax.rem(kr + 1 + j, G), c)).wait_send()

        @pl.when((r == nr) & (c == kr) & (k <= NBLK - 2))
        def _():
            cb_copy(k, 0, (bt, nr, nr)).wait_send()

            @pl.when(k <= NBLK - 3)
            def _():
                for j in range(1, G):
                    cb_copy(k, j, (bt, lax.rem(nr + j, G), nr)).wait_send()

        def each(q, carry):
            @pl.when((c == kr) & (k <= NBLK - 3))
            def _():
                for j in range(3):
                    rp_copy(k, q, j, (bt, r, lax.rem(kr + 1 + j, G))).wait_send()

            @pl.when(is_diag & (k <= NBLK - 4))
            def _():
                cp_copy(k, q, 0, (bt, dest_b, c)).wait_send()
                cp_copy(k, q, 1, (bt, dest_a, c)).wait_send()

            @pl.when(relays & (k <= NBLK - 4))
            def _():
                cp_copy(k, q, 0, (bt, dest_e, c)).wait_send()

            return carry

        return lax.fori_loop(p, NCH, each, carry)

    lax.fori_loop(0, NBLK, drain, 0)

    for t in range(NLOC):
        here = slice(t * B, (t + 1) * B)
        if t + 1 < NLOC:
            s_ref[here, (t + 1) * B:] = jnp.zeros((B, (NLOC - 1 - t) * B), F32)

        @pl.when(r < c)
        def _():
            s_ref[here, here] = jnp.zeros((B, B), F32)

        @pl.when(is_diag)
        def _():
            s_ref[here, here] = ld[here, :]


def solution(mesh):
    n = NLOC * B
    panels = (NCH * (NCH + 1) // 2) * 12 * CR

    def local(a_loc):
        dma = pltpu.SemaphoreType.DMA
        out = pl.pallas_call(
            kernel,
            out_shape=jax.ShapeDtypeStruct((n, n), F32),
            in_specs=[pl.BlockSpec(memory_space=pl.ANY)],
            out_specs=pl.BlockSpec(memory_space=pltpu.VMEM),
            scratch_shapes=[
                pltpu.VMEM((panels, B), BF16),
                pltpu.VMEM((panels, B), BF16),
                pltpu.VMEM((NBLK * B, B), BF16),
                pltpu.VMEM((NBLK * B, B), F32),
                pltpu.VMEM((n, B), F32),
                pltpu.VMEM((B, B), F32),
                pltpu.VMEM((B, 6 * B), BF16),
                pltpu.VMEM((CR, B), BF16),
                dma(()),
                dma((NBLK,)),
                dma((NBLK * 3,)),
                dma((NBLK,)),
                dma((NBLK * 4,)),
                dma((NBLK * NCH,)),
                dma((NBLK * 3 * NCH,)),
                dma((NBLK * NCH,)),
                dma((NBLK * 2 * NCH,)),
            ],
            compiler_params=pltpu.CompilerParams(has_side_effects=True, vmem_limit_bytes=62 << 20),
        )(a_loc.reshape(n, n))
        return out.reshape(a_loc.shape)

    spec = P(("batch", "row"), None, "col")
    return jax.shard_map(local, mesh=mesh, in_specs=(spec,), out_specs=spec, check_vma=False)
```

```python
import functools
import jax
import jax.numpy as jnp
from jax import lax
from jax.experimental import pallas as pl
from jax.experimental.pallas import tpu as pltpu
from jax.sharding import PartitionSpec as P

B = 128
NBLK = 48
G = 4
NLOC = 12
CH = 3
NCH = NLOC // CH
CR = CH * B
PANEL = 32
MESH = pl.DeviceIdType.MESH
NT = (((1,), (1,)), ((), ()))
TN = (((0,), (0,)), ((), ()))
F32 = jnp.float32
BF16 = jnp.bfloat16


def split3(x):
    hi = x.astype(BF16)
    rest = x - hi.astype(F32)
    mid = rest.astype(BF16)
    low = (rest - mid.astype(F32)).astype(BF16)
    return hi, mid, low


def left6(x, axis):
    hi, mid, low = split3(x)
    return jnp.concatenate([hi, mid, low, hi, mid, hi], axis=axis)


def right6(x, axis):
    hi, mid, low = split3(x)
    return jnp.concatenate([low, mid, hi, mid, hi, hi], axis=axis)


def dot(a, b, dims):
    return lax.dot_general(a, b, dims, preferred_element_type=F32)


def factor_panel(w, lane0):
    n = w.shape[0]
    cols = jnp.stack([jnp.broadcast_to(w[:, lane0 + j:lane0 + j + 1], (n, B)) for j in range(n)])
    sub = lax.broadcasted_iota(jnp.int32, (8, 2 * B), 0)
    groups = [w[8 * g:8 * g + 8] for g in range(n // 8)]
    scales = [jnp.zeros((8, 2 * B), F32) for g in range(n // 8)]

    def twice(v):
        return jnp.concatenate([v, v], axis=1)

    for j in range(n):
        g0, s = j // 8, j % 8
        if s == 0 and j:
            cols = cols[:, 8:]
        col = cols[0]
        pivot = col[s:s + 1]
        fac = col * (1.0 / pivot)
        if j + 1 < n:
            cols = cols[1:] - fac[None] * col[s + 1:, None, :]
        fac2 = twice(fac)
        row = groups[g0][s:s + 1]
        scales[g0] = jnp.where(sub == s, twice(lax.rsqrt(pivot)), scales[g0])
        if s < 7:
            groups[g0] = groups[g0] - jnp.where(sub > s, fac2[:8], 0.0) * row
        for g in range(g0 + 1, n // 8):
            groups[g] = groups[g] - fac2[8 * (g - g0):8 * (g - g0) + 8] * row
    return jnp.concatenate([g * f for g, f in zip(groups, scales)], axis=0)


def factor_block(a):
    r = lax.broadcasted_iota(jnp.int32, (B, B), 0)
    c = lax.broadcasted_iota(jnp.int32, (B, B), 1)
    w = jnp.concatenate([a, jnp.where(r == c, 1.0, 0.0).astype(F32)], axis=1)
    done = []
    for p in range(B // PANEL):
        f = factor_panel(w[:PANEL], PANEL * p)
        done.append(f)
        if p + 1 < B // PANEL:
            w = w[PANEL:] - dot(left6(f[:, :B], 0), right6(f, 0), TN)[PANEL * (p + 1):]
    f = jnp.concatenate(done, axis=0)
    return f[:, :B], f[:, B:]


SPREAD = ((0, 1, 1, 0), (0, 2, 2, 0), (0, 3, 3, 0), (1, 0, 2, 1), (1, 0, 0, 1), (1, 0, 3, 1),
          (2, 3, 1, 2), (2, 3, 3, 2), (2, 3, 0, 2), (3, 2, 2, 3), (3, 1, 1, 3), (3, 0, 0, 3))


def kernel(a_ref, s_ref, rp, cp, cb, linv, ld, a_s, mcat, rhs_s, last_s, in_sem,
           inv_r, inv_s, cb_r, cb_s, rp_r, rp_s, cp_r, cp_s):
    bt = lax.axis_index("batch")
    r = lax.axis_index("row")
    c = lax.axis_index("col")

    def rows(i, n=B):
        return pl.ds(pl.multiple_of(i * B, B), n)

    def phase(k):
        return lax.div(k, 12)

    def base(k):
        p = phase(k)
        return 144 * p - 18 * p * (p - 1) + (k - 12 * p) * (12 - 3 * p)

    def chunk(k, q):
        return rows(base(k) + CH * (q - phase(k)), CR)

    def rcopy(buf, where, ssem, rsem, dev):
        return pltpu.make_async_remote_copy(
            src_ref=buf.at[where, :], dst_ref=buf.at[where, :], send_sem=ssem, recv_sem=rsem,
            device_id=dev, device_id_type=MESH)

    def inv_copy(k, j, dev):
        return rcopy(linv, rows(k), inv_s.at[k * 3 + j], inv_r.at[k], dev)

    def cb_copy(k, j, dev):
        return rcopy(cb, rows(k), cb_s.at[k * 4 + j], cb_r.at[k], dev)

    def rp_copy(k, q, j, dev):
        return rcopy(rp, chunk(k, q), rp_s.at[(k * 3 + j) * NCH + q], rp_r.at[k * NCH + q], dev)

    def cp_copy(k, q, j, dev):
        return pltpu.make_async_remote_copy(
            src_ref=rp.at[chunk(k, q), :], dst_ref=cp.at[chunk(k, q), :],
            send_sem=cp_s.at[(k * 3 + j) * NCH + q], recv_sem=cp_r.at[k * NCH + q],
            device_id=dev, device_id_type=MESH)

    def spread(k, q, act):
        count = {}
        for sr, sc, dr, dc in SPREAD:
            j = count.get((sr, sc), 0)
            count[(sr, sc)] = j + 1

            @pl.when((r == sr) & (c == sc))
            def _():
                act(cp_copy(k, q, j, (bt, dr, dc)))

    is_diag = r == c

    def row_target(kr, j):
        twin = kr + 1 - 2 * lax.rem(kr, 2)
        entry = 2 - 2 * lax.div(kr, 2)
        first_twin = lax.rem(kr, 2) == 0
        return jnp.where(first_twin, twin, entry) if j == 0 else jnp.where(first_twin, entry, twin)

    def passes_on(kr):
        return c == 2 - 2 * lax.div(kr, 2)

    load = pltpu.make_async_copy(a_ref, s_ref, in_sem)
    load.start()
    load.wait()

    def step(it, carry):
        k = it - 1
        kk = jnp.maximum(k, 0)
        kr = lax.rem(kk, G)
        nr = lax.rem(it, G)
        p = phase(kk)
        tk = lax.div(kk, G)
        tn = lax.div(it, G)

        @pl.when((k >= 0) & (c == kr))
        def _():
            @pl.when(r != kr)
            def _():
                inv_copy(kk, 0, (bt, kr, c)).wait_recv()

            mcat[...] = right6(linv[rows(kk), :], 1)

            @pl.when(r == nr)
            def _():
                x = dot(left6(s_ref[rows(tn), rows(tk)], 1), mcat[...], NT)
                cb[rows(kk), :] = x.astype(BF16)
                cb_copy(kk, 0, (bt, nr, nr)).start()

                @pl.when(k <= NBLK - 3)
                def _():
                    for j in range(1, G):
                        cb_copy(kk, j, (bt, lax.rem(nr + j, G), nr)).start()

            def solve(q, carry):
                x = s_ref[rows(CH * q, CR), rows(tk)]
                y = dot(left6(x, 1), mcat[...], NT)
                t = lax.broadcasted_iota(jnp.int32, (CR, B), 0) // B + CH * q
                below = t * G + r > kk
                s_ref[rows(CH * q, CR), rows(tk)] = jnp.where(below, y, x)
                rp[chunk(kk, q), :] = jnp.where(below, y, 0.0).astype(BF16)

                @pl.when(k <= NBLK - 3)
                def _():
                    for j in range(2):
                        rp_copy(kk, q, j, (bt, r, row_target(kr, j))).start()

                return carry

            lax.fori_loop(p, NCH, solve, 0)

        @pl.when((r == nr) & (c == nr))
        def _():
            a_s[...] = s_ref[rows(tn), rows(tn)]

            for back in (2, 1):
                @pl.when(k >= back)
                def _():
                    kp = jnp.maximum(k - back, 0)
                    blk = rp[rows(base(kp) + tn - CH * phase(kp)), :]
                    a_s[...] -= dot(blk, blk, NT)

            @pl.when(k >= 0)
            def _():
                cb_copy(kk, 0, (bt, r, kr)).wait_recv()
                blk = cb[rows(kk), :]
                a_s[...] -= dot(blk, blk, NT)

            u, m = factor_block(a_s[...])
            linv[rows(it), :] = m

            @pl.when(it < NBLK - 1)
            def _():
                for j in range(3):
                    inv_copy(it, j, (bt, lax.rem(nr + 1 + j, G), c)).start()

            low = jnp.transpose(u)
            i0 = lax.broadcasted_iota(jnp.int32, (B, B), 0)
            i1 = lax.broadcasted_iota(jnp.int32, (B, B), 1)
            ld[rows(tn), :] = jnp.where(i0 >= i1, low, 0.0)

        @pl.when((k >= 0) & (k <= NBLK - 3))
        def _():
            @pl.when((c == nr) & (r != nr))
            def _():
                cb_copy(kk, 0, (bt, nr, kr)).wait_recv()

            k1 = jnp.maximum(k - 1, 0)
            qn = lax.div(tn, CH)

            @pl.when((c == nr) & (k >= 1))
            def _():
                @pl.when(is_diag)
                def _():
                    last_s[...] = rp[rows(base(k1) + tn - CH * phase(k1)), :]

                @pl.when(jnp.logical_not(is_diag))
                def _():
                    cp_copy(k1, qn, 0, (bt, r, c)).wait_recv()
                    last_s[...] = cp[rows(base(k1) + tn - CH * phase(k1)), :]

                def catch_up(q, carry):
                    s_ref[rows(CH * q, CR), rows(tn)] -= dot(rp[chunk(k1, q), :], last_s[...], NT)
                    return carry

                lax.fori_loop(p, NCH, catch_up, 0)

            def take(q, carry):
                @pl.when(c != kr)
                def _():
                    rp_copy(kk, q, 0, (bt, r, kr)).wait_recv()

                @pl.when(passes_on(kr))
                def _():
                    rp_copy(kk, q, 2, (bt, r, c + 1)).start()

                @pl.when(k <= NBLK - 4)
                def _():
                    spread(kk, q, lambda copy: copy.start())

                @pl.when(c == nr)
                def _():
                    s_ref[rows(CH * q, CR), rows(tn)] -= dot(rp[chunk(kk, q), :], cb[rows(kk), :], NT)

                return carry

            lax.fori_loop(p, NCH, take, 0)

        @pl.when(k >= 2)
        def _():
            kp = jnp.maximum(k - 2, 0)
            k1 = jnp.maximum(k - 1, 0)
            pp = phase(kp)
            t1 = lax.div(k1, G)

            def by_col(cq, carry):
                @pl.when(is_diag)
                def _():
                    rhs_s[...] = rp[chunk(kp, cq), :]

                @pl.when(jnp.logical_not(is_diag))
                def _():
                    @pl.when(jnp.logical_not((c == kr) & (lax.div(tk, CH) == cq)))
                    def _():
                        cp_copy(kp, cq, 0, (bt, r, c)).wait_recv()

                    rhs_s[...] = cp[chunk(kp, cq), :]

                @pl.when((c == kr) & (lax.div(tk, CH) == cq))
                def _():
                    rhs_s[rows(lax.rem(tk, CH)), :] = jnp.zeros((B, B), BF16)

                @pl.when((c == lax.rem(k1, G)) & (lax.div(t1, CH) == cq))
                def _():
                    rhs_s[rows(lax.rem(t1, CH)), :] = jnp.zeros((B, B), BF16)

                def by_row(rq, carry):
                    s_ref[rows(CH * rq, CR), rows(CH * cq, CR)] -= dot(rp[chunk(kp, rq), :], rhs_s[...], NT)
                    return carry

                return lax.fori_loop(cq, NCH, by_row, carry)

            lax.fori_loop(pp, NCH, by_col, 0)

        return carry

    lax.fori_loop(0, NBLK, step, 0)

    def drain(k, carry):
        kr = lax.rem(k, G)
        nr = lax.rem(k + 1, G)
        p = phase(k)

        @pl.when((r == kr) & (c == kr) & (k < NBLK - 1))
        def _():
            for j in range(3):
                inv_copy(k, j, (bt, lax.rem(kr + 1 + j, G), c)).wait_send()

        @pl.when((r == nr) & (c == kr) & (k <= NBLK - 2))
        def _():
            cb_copy(k, 0, (bt, nr, nr)).wait_send()

            @pl.when(k <= NBLK - 3)
            def _():
                for j in range(1, G):
                    cb_copy(k, j, (bt, lax.rem(nr + j, G), nr)).wait_send()

        def each(q, carry):
            @pl.when((c == kr) & (k <= NBLK - 3))
            def _():
                for j in range(2):
                    rp_copy(k, q, j, (bt, r, row_target(kr, j))).wait_send()

            @pl.when(passes_on(kr) & (k <= NBLK - 3))
            def _():
                rp_copy(k, q, 2, (bt, r, c + 1)).wait_send()

            @pl.when(k <= NBLK - 4)
            def _():
                spread(k, q, lambda copy: copy.wait_send())

            return carry

        return lax.fori_loop(p, NCH, each, carry)

    lax.fori_loop(0, NBLK, drain, 0)

    for t in range(NLOC):
        here = slice(t * B, (t + 1) * B)
        if t + 1 < NLOC:
            s_ref[here, (t + 1) * B:] = jnp.zeros((B, (NLOC - 1 - t) * B), F32)

        @pl.when(r < c)
        def _():
            s_ref[here, here] = jnp.zeros((B, B), F32)

        @pl.when(is_diag)
        def _():
            s_ref[here, here] = ld[here, :]


def solution(mesh):
    n = NLOC * B
    panels = (NCH * (NCH + 1) // 2) * 12 * CR

    def local(a_loc):
        dma = pltpu.SemaphoreType.DMA
        out = pl.pallas_call(
            kernel,
            out_shape=jax.ShapeDtypeStruct((n, n), F32),
            in_specs=[pl.BlockSpec(memory_space=pl.ANY)],
            out_specs=pl.BlockSpec(memory_space=pltpu.VMEM),
            scratch_shapes=[
                pltpu.VMEM((panels, B), BF16),
                pltpu.VMEM((panels, B), BF16),
                pltpu.VMEM((NBLK * B, B), BF16),
                pltpu.VMEM((NBLK * B, B), F32),
                pltpu.VMEM((n, B), F32),
                pltpu.VMEM((B, B), F32),
                pltpu.VMEM((B, 6 * B), BF16),
                pltpu.VMEM((CR, B), BF16),
                pltpu.VMEM((B, B), BF16),
                dma(()),
                dma((NBLK,)),
                dma((NBLK * 3,)),
                dma((NBLK,)),
                dma((NBLK * 4,)),
                dma((NBLK * NCH,)),
                dma((NBLK * 3 * NCH,)),
                dma((NBLK * NCH,)),
                dma((NBLK * 3 * NCH,)),
            ],
            compiler_params=pltpu.CompilerParams(has_side_effects=True, vmem_limit_bytes=62 << 20),
        )(a_loc.reshape(n, n))
        return out.reshape(a_loc.shape)

    spec = P(("batch", "row"), None, "col")
    return jax.shard_map(local, mesh=mesh, in_specs=(spec,), out_specs=spec, check_vma=False)
```

```python
import functools
import jax
import jax.numpy as jnp
from jax import lax
from jax.experimental import pallas as pl
from jax.experimental.pallas import tpu as pltpu
from jax.sharding import PartitionSpec as P

B = 128
NBLK = 48
G = 4
NLOC = 12
CH = 3
NCH = NLOC // CH
CR = CH * B
PANEL = 32
MESH = pl.DeviceIdType.MESH
NT = (((1,), (1,)), ((), ()))
TN = (((0,), (0,)), ((), ()))
F32 = jnp.float32
BF16 = jnp.bfloat16


def split3(x):
    hi = x.astype(BF16)
    rest = x - hi.astype(F32)
    mid = rest.astype(BF16)
    low = (rest - mid.astype(F32)).astype(BF16)
    return hi, mid, low


def left6(x, axis):
    hi, mid, low = split3(x)
    return jnp.concatenate([hi, mid, low, hi, mid, hi], axis=axis)


def right6(x, axis):
    hi, mid, low = split3(x)
    return jnp.concatenate([low, mid, hi, mid, hi, hi], axis=axis)


def dot(a, b, dims):
    return lax.dot_general(a, b, dims, preferred_element_type=F32)


def factor_panel(w, lane0):
    n = w.shape[0]
    cols = jnp.stack([jnp.broadcast_to(w[:, lane0 + j:lane0 + j + 1], (n, B)) for j in range(n)])
    sub = lax.broadcasted_iota(jnp.int32, (8, 2 * B), 0)
    groups = [w[8 * g:8 * g + 8] for g in range(n // 8)]
    scales = [jnp.zeros((8, 2 * B), F32) for g in range(n // 8)]

    def twice(v):
        return jnp.concatenate([v, v], axis=1)

    for j in range(n):
        g0, s = j // 8, j % 8
        if s == 0 and j:
            cols = cols[:, 8:]
        col = cols[0]
        pivot = col[s:s + 1]
        fac = col * (1.0 / pivot)
        if j + 1 < n:
            cols = cols[1:] - fac[None] * col[s + 1:, None, :]
        fac2 = twice(fac)
        row = groups[g0][s:s + 1]
        scales[g0] = jnp.where(sub == s, twice(lax.rsqrt(pivot)), scales[g0])
        if s < 7:
            groups[g0] = groups[g0] - jnp.where(sub > s, fac2[:8], 0.0) * row
        for g in range(g0 + 1, n // 8):
            groups[g] = groups[g] - fac2[8 * (g - g0):8 * (g - g0) + 8] * row
    return jnp.concatenate([g * f for g, f in zip(groups, scales)], axis=0)


def factor_block(a):
    r = lax.broadcasted_iota(jnp.int32, (B, B), 0)
    c = lax.broadcasted_iota(jnp.int32, (B, B), 1)
    w = jnp.concatenate([a, jnp.where(r == c, 1.0, 0.0).astype(F32)], axis=1)
    done = []
    for p in range(B // PANEL):
        f = factor_panel(w[:PANEL], PANEL * p)
        done.append(f)
        if p + 1 < B // PANEL:
            w = w[PANEL:] - dot(left6(f[:, :B], 0), right6(f, 0), TN)[PANEL * (p + 1):]
    f = jnp.concatenate(done, axis=0)
    return f[:, :B], f[:, B:]


SPREAD = ((0, 1, 1, 0), (0, 2, 2, 0), (0, 3, 3, 0), (1, 0, 2, 1), (1, 0, 0, 1), (1, 0, 3, 1),
          (2, 3, 1, 2), (2, 3, 3, 2), (2, 3, 0, 2), (3, 2, 2, 3), (3, 1, 1, 3), (3, 0, 0, 3))


def kernel(a_ref, s_ref, rp, cp, cb, linv, ld, a_s, mcat, rhs_s, last_s, in_sem, first_sem,
           inv_r, inv_s, cb_r, cb_s, rp_r, rp_s, cp_r, cp_s):
    bt = lax.axis_index("batch")
    r = lax.axis_index("row")
    c = lax.axis_index("col")

    def rows(i, n=B):
        return pl.ds(pl.multiple_of(i * B, B), n)

    def phase(k):
        return lax.div(k, 12)

    def base(k):
        p = phase(k)
        return 144 * p - 18 * p * (p - 1) + (k - 12 * p) * (12 - 3 * p)

    def chunk(k, q):
        return rows(base(k) + CH * (q - phase(k)), CR)

    def rcopy(buf, where, ssem, rsem, dev):
        return pltpu.make_async_remote_copy(
            src_ref=buf.at[where, :], dst_ref=buf.at[where, :], send_sem=ssem, recv_sem=rsem,
            device_id=dev, device_id_type=MESH)

    def inv_copy(k, j, dev):
        return rcopy(linv, rows(k), inv_s.at[k * 3 + j], inv_r.at[k], dev)

    def cb_copy(k, j, dev):
        return rcopy(cb, rows(k), cb_s.at[k * 4 + j], cb_r.at[k], dev)

    def rp_copy(k, q, j, dev):
        return rcopy(rp, chunk(k, q), rp_s.at[(k * 3 + j) * NCH + q], rp_r.at[k * NCH + q], dev)

    def cp_copy(k, q, j, dev):
        return pltpu.make_async_remote_copy(
            src_ref=rp.at[chunk(k, q), :], dst_ref=cp.at[chunk(k, q), :],
            send_sem=cp_s.at[(k * 3 + j) * NCH + q], recv_sem=cp_r.at[k * NCH + q],
            device_id=dev, device_id_type=MESH)

    def spread(k, q, act):
        count = {}
        for sr, sc, dr, dc in SPREAD:
            j = count.get((sr, sc), 0)
            count[(sr, sc)] = j + 1

            @pl.when((r == sr) & (c == sc))
            def _():
                act(cp_copy(k, q, j, (bt, dr, dc)))

    is_diag = r == c

    def row_target(kr, j):
        twin = kr + 1 - 2 * lax.rem(kr, 2)
        entry = 2 - 2 * lax.div(kr, 2)
        first_twin = lax.rem(kr, 2) == 0
        return jnp.where(first_twin, twin, entry) if j == 0 else jnp.where(first_twin, entry, twin)

    def passes_on(kr):
        return c == 2 - 2 * lax.div(kr, 2)

    first = pltpu.make_async_copy(a_ref.at[0:B, 0:B], a_s, first_sem)
    first.start()
    load = pltpu.make_async_copy(a_ref, s_ref, in_sem)
    load.start()
    first.wait()

    def step(it, carry):
        k = it - 1
        kk = jnp.maximum(k, 0)
        kr = lax.rem(kk, G)
        nr = lax.rem(it, G)
        p = phase(kk)
        tk = lax.div(kk, G)
        tn = lax.div(it, G)

        @pl.when((k >= 0) & (c == kr))
        def _():
            @pl.when(r != kr)
            def _():
                inv_copy(kk, 0, (bt, kr, c)).wait_recv()

            mcat[...] = right6(linv[rows(kk), :], 1)

            @pl.when(r == nr)
            def _():
                x = dot(left6(s_ref[rows(tn), rows(tk)], 1), mcat[...], NT)
                cb[rows(kk), :] = x.astype(BF16)
                cb_copy(kk, 0, (bt, nr, nr)).start()

                @pl.when(k <= NBLK - 3)
                def _():
                    for j in range(1, G):
                        cb_copy(kk, j, (bt, lax.rem(nr + j, G), nr)).start()

            def solve(q, carry):
                x = s_ref[rows(CH * q, CR), rows(tk)]
                y = dot(left6(x, 1), mcat[...], NT)
                t = lax.broadcasted_iota(jnp.int32, (CR, B), 0) // B + CH * q
                below = t * G + r > kk
                s_ref[rows(CH * q, CR), rows(tk)] = jnp.where(below, y, x)
                rp[chunk(kk, q), :] = jnp.where(below, y, 0.0).astype(BF16)

                @pl.when(k <= NBLK - 3)
                def _():
                    for j in range(2):
                        rp_copy(kk, q, j, (bt, r, row_target(kr, j))).start()

                return carry

            lax.fori_loop(p, NCH, solve, 0)

        @pl.when((r == nr) & (c == nr))
        def _():
            @pl.when(it > 0)
            def _():
                a_s[...] = s_ref[rows(tn), rows(tn)]

            for back in (2, 1):
                @pl.when(k >= back)
                def _():
                    kp = jnp.maximum(k - back, 0)
                    blk = rp[rows(base(kp) + tn - CH * phase(kp)), :]
                    a_s[...] -= dot(blk, blk, NT)

            @pl.when(k >= 0)
            def _():
                cb_copy(kk, 0, (bt, r, kr)).wait_recv()
                blk = cb[rows(kk), :]
                a_s[...] -= dot(blk, blk, NT)

            u, m = factor_block(a_s[...])
            linv[rows(it), :] = m

            @pl.when(it < NBLK - 1)
            def _():
                for j in range(3):
                    inv_copy(it, j, (bt, lax.rem(nr + 1 + j, G), c)).start()

            low = jnp.transpose(u)
            i0 = lax.broadcasted_iota(jnp.int32, (B, B), 0)
            i1 = lax.broadcasted_iota(jnp.int32, (B, B), 1)
            ld[rows(tn), :] = jnp.where(i0 >= i1, low, 0.0)

        @pl.when(it == 0)
        def _():
            load.wait()

        @pl.when(k >= 2)
        def _():
            kp = jnp.maximum(k - 2, 0)
            k1 = jnp.maximum(k - 1, 0)
            pp = phase(kp)
            t1 = lax.div(k1, G)

            def by_col(cq, carry):
                @pl.when(is_diag)
                def _():
                    rhs_s[...] = rp[chunk(kp, cq), :]

                @pl.when(jnp.logical_not(is_diag))
                def _():
                    @pl.when(jnp.logical_not((c == kr) & (lax.div(tk, CH) == cq)))
                    def _():
                        cp_copy(kp, cq, 0, (bt, r, c)).wait_recv()

                    rhs_s[...] = cp[chunk(kp, cq), :]

                @pl.when((c == kr) & (lax.div(tk, CH) == cq))
                def _():
                    rhs_s[rows(lax.rem(tk, CH)), :] = jnp.zeros((B, B), BF16)

                @pl.when((c == lax.rem(k1, G)) & (lax.div(t1, CH) == cq))
                def _():
                    rhs_s[rows(lax.rem(t1, CH)), :] = jnp.zeros((B, B), BF16)

                def by_row(rq, carry):
                    s_ref[rows(CH * rq, CR), rows(CH * cq, CR)] -= dot(rp[chunk(kp, rq), :], rhs_s[...], NT)
                    return carry

                return lax.fori_loop(cq, NCH, by_row, carry)

            lax.fori_loop(pp, NCH, by_col, 0)

        @pl.when((k >= 0) & (k <= NBLK - 3))
        def _():
            @pl.when((c == nr) & (r != nr))
            def _():
                cb_copy(kk, 0, (bt, nr, kr)).wait_recv()

            k1 = jnp.maximum(k - 1, 0)
            qn = lax.div(tn, CH)

            @pl.when((c == nr) & (k >= 1))
            def _():
                @pl.when(is_diag)
                def _():
                    last_s[...] = rp[rows(base(k1) + tn - CH * phase(k1)), :]

                @pl.when(jnp.logical_not(is_diag))
                def _():
                    cp_copy(k1, qn, 0, (bt, r, c)).wait_recv()
                    last_s[...] = cp[rows(base(k1) + tn - CH * phase(k1)), :]

                def catch_up(q, carry):
                    s_ref[rows(CH * q, CR), rows(tn)] -= dot(rp[chunk(k1, q), :], last_s[...], NT)
                    return carry

                lax.fori_loop(p, NCH, catch_up, 0)

            def take(q, carry):
                @pl.when(c != kr)
                def _():
                    rp_copy(kk, q, 0, (bt, r, kr)).wait_recv()

                @pl.when(passes_on(kr))
                def _():
                    rp_copy(kk, q, 2, (bt, r, c + 1)).start()

                @pl.when(c == nr)
                def _():
                    s_ref[rows(CH * q, CR), rows(tn)] -= dot(rp[chunk(kk, q), :], cb[rows(kk), :], NT)

                @pl.when(k <= NBLK - 4)
                def _():
                    spread(kk, q, lambda copy: copy.start())

                return carry

            lax.fori_loop(p, NCH, take, 0)

        return carry

    lax.fori_loop(0, NBLK, step, 0)

    def drain(k, carry):
        kr = lax.rem(k, G)
        nr = lax.rem(k + 1, G)
        p = phase(k)

        @pl.when((r == kr) & (c == kr) & (k < NBLK - 1))
        def _():
            for j in range(3):
                inv_copy(k, j, (bt, lax.rem(kr + 1 + j, G), c)).wait_send()

        @pl.when((r == nr) & (c == kr) & (k <= NBLK - 2))
        def _():
            cb_copy(k, 0, (bt, nr, nr)).wait_send()

            @pl.when(k <= NBLK - 3)
            def _():
                for j in range(1, G):
                    cb_copy(k, j, (bt, lax.rem(nr + j, G), nr)).wait_send()

        def each(q, carry):
            @pl.when((c == kr) & (k <= NBLK - 3))
            def _():
                for j in range(2):
                    rp_copy(k, q, j, (bt, r, row_target(kr, j))).wait_send()

            @pl.when(passes_on(kr) & (k <= NBLK - 3))
            def _():
                rp_copy(k, q, 2, (bt, r, c + 1)).wait_send()

            @pl.when(k <= NBLK - 4)
            def _():
                spread(k, q, lambda copy: copy.wait_send())

            return carry

        return lax.fori_loop(p, NCH, each, carry)

    lax.fori_loop(0, NBLK, drain, 0)

    for t in range(NLOC):
        here = slice(t * B, (t + 1) * B)
        if t + 1 < NLOC:
            s_ref[here, (t + 1) * B:] = jnp.zeros((B, (NLOC - 1 - t) * B), F32)

        @pl.when(r < c)
        def _():
            s_ref[here, here] = jnp.zeros((B, B), F32)

        @pl.when(is_diag)
        def _():
            s_ref[here, here] = ld[here, :]


def solution(mesh):
    n = NLOC * B
    panels = (NCH * (NCH + 1) // 2) * 12 * CR

    def local(a_loc):
        dma = pltpu.SemaphoreType.DMA
        out = pl.pallas_call(
            kernel,
            out_shape=jax.ShapeDtypeStruct((n, n), F32),
            in_specs=[pl.BlockSpec(memory_space=pl.ANY)],
            out_specs=pl.BlockSpec(memory_space=pltpu.VMEM),
            scratch_shapes=[
                pltpu.VMEM((panels, B), BF16),
                pltpu.VMEM((panels, B), BF16),
                pltpu.VMEM((NBLK * B, B), BF16),
                pltpu.VMEM((NBLK * B, B), F32),
                pltpu.VMEM((n, B), F32),
                pltpu.VMEM((B, B), F32),
                pltpu.VMEM((B, 6 * B), BF16),
                pltpu.VMEM((CR, B), BF16),
                pltpu.VMEM((B, B), BF16),
                dma(()),
                dma(()),
                dma((NBLK,)),
                dma((NBLK * 3,)),
                dma((NBLK,)),
                dma((NBLK * 4,)),
                dma((NBLK * NCH,)),
                dma((NBLK * 3 * NCH,)),
                dma((NBLK * NCH,)),
                dma((NBLK * 3 * NCH,)),
            ],
            compiler_params=pltpu.CompilerParams(has_side_effects=True, vmem_limit_bytes=62 << 20),
        )(a_loc.reshape(n, n))
        return out.reshape(a_loc.shape)

    spec = P(("batch", "row"), None, "col")
    return jax.shard_map(local, mesh=mesh, in_specs=(spec,), out_specs=spec, check_vma=False)
```
